32 devices in a mesh: dp: 1 (over z), sp: 4 (over y), cp: 8 (over x, core).
Axes of the slice: x: 4, y: 4, z: 1, core: 2. Of those that a mesh axis runs over, the one named last changes fastest.
The devices are a block of a 4x4x8 slice.
Arguments:
- hidden: bfloat16 [8, 4096, 3072], P('dp', ('cp', 'sp'))
- seg_ids: int32 [8, 4096], P('dp', ('cp', 'sp'))
- w_qkv: bfloat16 [3072, 3, 24, 128], replicated
- w_out: bfloat16 [24, 128, 3072], replicated
Outputs:
- output: bfloat16 [8, 4096, 3072], P('dp', ('cp', 'sp'))
All inputs are finite; a program needn't handle non-finite values.
Results may differ from the reference program's by a relative error of at most 0.00599118.
Values are sent between devices in bfloat16 or wider.
A program may use at most 768 MiB of HBM per device.

```python
import jax
import jax.numpy as jnp
from jax import lax

BATCH = 8
SEQ = 4096
DIM = 3072
HEADS = 24
HEAD = 128
QUERY_BLOCK = 256
CUTS = 3


def draw_segments(seg_key):
    key_first, key_rest = jax.random.split(seg_key)
    first_cut = jax.random.randint(key_first, (BATCH, 1), SEQ // 2 + SEQ // 8, SEQ - SEQ // 8)
    offsets = jax.random.randint(key_rest, (BATCH, CUTS - 1), 0, 1 << 20) % (SEQ - first_cut)
    cut_points = jnp.concatenate([first_cut, first_cut + offsets], axis=1)
    positions = jnp.arange(SEQ, dtype=jnp.int32)
    return jnp.sum(positions[None, :, None] >= cut_points[:, None, :], axis=-1).astype(jnp.int32)


def setup_inputs(seed: int = 0, part: int = 0) -> dict:
    part_key = jax.random.fold_in(jax.random.key(seed), part)
    key_hidden, key_seg = jax.random.split(part_key)
    key_qkv, key_out = jax.random.split(jax.random.key(seed + 1))
    hidden = jax.random.normal(key_hidden, (BATCH, SEQ, DIM), jnp.float32)
    qkv_gain = jnp.where(jnp.arange(3) < 2, (2.0 / DIM) ** 0.5, DIM ** -0.5)
    w_qkv = jax.random.normal(key_qkv, (DIM, 3, HEADS, HEAD), jnp.float32) * qkv_gain[:, None, None]
    out_gain = (HEADS * HEAD) ** -0.5 * SEQ ** 0.5 / 10.0
    w_out = jax.random.normal(key_out, (HEADS, HEAD, DIM), jnp.float32) * out_gain
    return {'hidden': hidden.astype(jnp.bfloat16), 'seg_ids': draw_segments(key_seg), 'w_qkv': w_qkv.astype(jnp.bfloat16), 'w_out': w_out.astype(jnp.bfloat16)}


def reference(hidden, seg_ids, w_qkv, w_out):
    projected = jnp.dot(hidden.reshape(BATCH * SEQ, DIM), w_qkv.reshape(DIM, 3 * HEADS * HEAD), preferred_element_type=jnp.float32)
    projected = projected.astype(jnp.bfloat16).reshape(BATCH, SEQ, 3, HEADS, HEAD)
    per_head = jnp.transpose(projected, (3, 2, 0, 1, 4))
    num_blocks = SEQ // QUERY_BLOCK
    seg_blocks = jnp.transpose(seg_ids.reshape(BATCH, num_blocks, QUERY_BLOCK), (1, 0, 2))
    logit_scale = HEAD ** -0.5

    def one_head(head_qkv):
        keys_f32 = head_qkv[1].astype(jnp.float32)
        values_f32 = head_qkv[2].astype(jnp.float32)
        query_blocks = jnp.transpose(head_qkv[0].reshape(BATCH, num_blocks, QUERY_BLOCK, HEAD), (1, 0, 2, 3))

        def one_block(block_args):
            query_blk, seg_blk = block_args
            scores = jnp.einsum('bqd,bkd->bqk', query_blk.astype(jnp.float32), keys_f32) * logit_scale
            allowed = seg_blk[:, :, None] == seg_ids[:, None, :]
            scores = jnp.where(allowed, scores, -jnp.inf)
            row_max = jnp.max(scores, axis=-1, keepdims=True)
            weights = jnp.exp(scores - row_max)
            row_sum = jnp.sum(weights, axis=-1, keepdims=True)
            mixed_vals = jnp.einsum('bqk,bkd->bqd', weights.astype(jnp.bfloat16).astype(jnp.float32), values_f32)
            return (mixed_vals / row_sum).astype(jnp.bfloat16)

        out_blocks = lax.map(one_block, (query_blocks, seg_blocks))
        return jnp.transpose(out_blocks, (1, 0, 2, 3)).reshape(BATCH, SEQ, HEAD)

    attn_heads = lax.map(one_head, per_head)
    attn_flat = jnp.transpose(attn_heads, (1, 2, 0, 3)).reshape(BATCH * SEQ, HEADS * HEAD)
    result = jnp.dot(attn_flat, w_out.reshape(HEADS * HEAD, DIM), preferred_element_type=jnp.float32)
    return result.astype(jnp.bfloat16).reshape(BATCH, SEQ, DIM)
```

```python
import functools
import math

import jax
import jax.numpy as jnp
from jax import lax
from jax.experimental import pallas as pl
from jax.experimental.pallas import tpu as pltpu
from jax.sharding import PartitionSpec as P

MESH = pl.DeviceIdType.MESH
NEG = -3.3e38
CORES = 2


def place(rank, lane):
    return rank // CORES, rank % CORES, lane // 2, lane % 2


def gather_project_kernel(cols, hid, w_hbm, out, blocks, w_vmem, stage, recv_sem, direct_sem, relay_sem, twin_sem,
                          w_sem, own_sem, out_sem):
    rank, lane = lax.axis_index('cp'), lax.axis_index('sp')
    columns = cols
    x, core, pair, end = place(rank, lane)
    far = 3 - lane
    mate = 2 * pair + 1 - end

    def dev(xx, cc, yy):
        return {'cp': xx * CORES + cc, 'sp': yy}

    def slot_of(xx, hh, cc, ee):
        return ((xx * 2 + hh) * CORES + cc) * 2 + ee

    me = slot_of(x, pair, core, end)
    steps = [(dx, other) for dx in (0, 1, columns - 1, 2) for other in (0, 1)]
    twin = dev(x, 1 - core, lane)
    partner = dev(x, core, mate)

    barrier = pltpu.get_barrier_semaphore()
    targets = [dev((x + columns - dx) % columns, core, far if other else lane) for dx, other in steps[1:]]
    for target in targets + [partner, twin]:
        pl.semaphore_signal(barrier, inc=1, device_id=target, device_id_type=MESH)

    own_seq = x * 2 + pair
    own = pltpu.make_async_copy(hid.at[own_seq], blocks.at[me], own_sem)
    own.start()
    w_copy = pltpu.make_async_copy(w_hbm, w_vmem, w_sem)
    w_copy.start()
    pl.semaphore_wait(barrier, len(targets) + 2)

    directs = []
    for i, (dx, other) in enumerate(steps[1:]):
        xt = (x + columns - dx) % columns
        seq = xt * 2 + (1 - pair if other else pair)
        copy = pltpu.make_async_remote_copy(
            src_ref=hid.at[seq], dst_ref=blocks.at[me], send_sem=direct_sem.at[i], recv_sem=recv_sem.at[me],
            device_id=targets[i], device_id_type=MESH)
        copy.start()
        directs.append(copy)

    def remote(slot, sem, device):
        return pltpu.make_async_remote_copy(
            src_ref=blocks.at[slot], dst_ref=blocks.at[slot], send_sem=sem, recv_sem=recv_sem.at[slot],
            device_id=device, device_id_type=MESH)

    own.wait()
    rows = stage.shape[1] // 4
    depth, width = w_vmem.shape
    tile = 256

    def out_copies(j, xs, hs):
        buf = j % 2
        return [pltpu.make_async_copy(
            stage.at[buf, pl.ds(k * rows, rows)],
            out.at[pl.ds(pl.multiple_of(((xs * CORES + k // 2) * 4 + hs * 2 + k % 2) * rows, rows), rows)],
            out_sem.at[buf, k]) for k in range(4)]

    def group(j):
        s = j // 2
        dx = s + jnp.where(s == 2, 1, 0) - jnp.where(s == 3, 1, 0)
        xs = (x + dx) % columns
        hs = (pair + j % 2) % 2
        return xs, hs

    def step(j, carry):
        xs, hs = group(j)
        de = jnp.where(j % 2 == 0, end, 1 - end)
        direct = slot_of(xs, hs, core, de)
        via = slot_of(xs, hs, core, 1 - de)

        @pl.when(j > 0)
        def _():
            remote(direct, relay_sem.at[j], partner).wait_recv()

        remote(direct, relay_sem.at[j], partner).start()
        remote(direct, twin_sem.at[j, 0], twin).start()
        remote(via, twin_sem.at[j, 1], twin).wait_recv()
        remote(via, twin_sem.at[j, 1], twin).start()
        remote(slot_of(xs, hs, 1 - core, de), twin_sem.at[j, 0], twin).wait_recv()
        remote(slot_of(xs, hs, 1 - core, 1 - de), twin_sem.at[j, 1], twin).wait_recv()

        @pl.when(j == 0)
        def _():
            w_copy.wait()

        @pl.when(j >= 2)
        def _():
            for copy in out_copies(j, *group(j - 2)):
                copy.wait()

        base = slot_of(xs, hs, 0, 0)
        lhs = blocks.at[pl.ds(base, 4)]
        buf = j % 2

        def column(n, carry):
            c = pl.ds(pl.multiple_of(n * tile, tile), tile)
            acc = jnp.dot(lhs[...].reshape(4 * rows, depth), w_vmem[:, c], preferred_element_type=jnp.float32)
            stage[buf, :, c] = acc.astype(jnp.bfloat16)
            return carry

        lax.fori_loop(0, width // tile, column, 0)
        for copy in out_copies(j, xs, hs):
            copy.start()
        return carry

    n_groups = len(steps)
    lax.fori_loop(0, n_groups, step, 0)

    for copy in directs:
        copy.wait_send()

    def drain(j, carry):
        xs, hs = group(j)
        remote(me, relay_sem.at[j], partner).wait_send()
        remote(me, twin_sem.at[j, 0], twin).wait_send()
        remote(me, twin_sem.at[j, 1], twin).wait_send()

        @pl.when(j >= n_groups - 2)
        def _():
            for copy in out_copies(j, xs, hs):
                copy.wait()

        return carry

    lax.fori_loop(0, n_groups, drain, 0)


def gather_project(hidden, w_local, columns, n_blocks):
    batch, tokens, depth = hidden.shape
    width = w_local.shape[1]
    n_groups = n_blocks // 4
    return pl.pallas_call(
        functools.partial(gather_project_kernel, columns),
        out_shape=jax.ShapeDtypeStruct((n_blocks * tokens, width), jnp.bfloat16),
        in_specs=[pl.BlockSpec(memory_space=pl.ANY)] * 2,
        out_specs=pl.BlockSpec(memory_space=pl.ANY),
        scratch_shapes=[
            pltpu.VMEM((n_blocks, tokens, depth), jnp.bfloat16),
            pltpu.VMEM((depth, width), jnp.bfloat16),
            pltpu.VMEM((2, 4 * tokens, width), jnp.bfloat16),
            pltpu.SemaphoreType.DMA((n_blocks,)),
            pltpu.SemaphoreType.DMA((n_groups - 1,)),
            pltpu.SemaphoreType.DMA((n_groups,)),
            pltpu.SemaphoreType.DMA((n_groups, 2)),
            pltpu.SemaphoreType.DMA,
            pltpu.SemaphoreType.DMA,
            pltpu.SemaphoreType.DMA((2, 4)),
        ],
        compiler_params=pltpu.CompilerParams(collective_id=0, has_side_effects=True, vmem_limit_bytes=60 * 2**20),
        name='gather_project',
    )(hidden, w_local)


def attention_kernel(tk, scale2, bounds, q_ref, k_ref, v_ref, segq_ref, segk_ref, o_ref, vt, s_buf):
    i = pl.program_id(1)
    tq, head_dim = q_ref.shape

    @pl.when(i == 0)
    def _():
        vt[...] = v_ref[...].T

    lo, full_lo, full_hi, hi = (bounds[n, i] for n in range(4))
    q = q_ref[...]

    def scores(chunk, slot):
        k = k_ref[pl.ds(pl.multiple_of(chunk * tk, tk), tk), :]
        s_buf[slot] = lax.dot_general(k, q, (((1,), (1,)), ((), ())), preferred_element_type=jnp.float32)

    def absorb(chunk, slot, state, masked):
        m, l, acc = state
        at = pl.ds(pl.multiple_of(chunk * tk, tk), tk)
        s = s_buf[slot]
        if masked:
            allowed = segk_ref[at, :1] == segq_ref[:1, :]
            s = jnp.where(allowed, s, NEG)
        m_new = jnp.maximum(m, jnp.max(s, axis=0, keepdims=True))
        p = jnp.exp2((s - m_new) * scale2)
        if masked:
            p = jnp.where(allowed, p, 0.0)
        alpha = jnp.exp2((m - m_new) * scale2)
        l = l * alpha + jnp.sum(p, axis=0, keepdims=True)
        acc = acc * alpha + lax.dot_general(vt[:, at], p.astype(jnp.bfloat16), (((1,), (0,)), ((), ())),
                                            preferred_element_type=jnp.float32)
        return m_new, l, acc

    head = full_lo - lo
    n_masked = head + hi - full_hi

    def masked_step(n, state):
        chunk = jnp.where(n < head, lo + n, full_hi + n - head)
        scores(chunk, 0)
        return absorb(chunk, 0, state, True)

    def full_step(n, state):
        slot = (n - full_lo) % 2

        scores(jnp.minimum(n + 1, full_hi - 1), 1 - slot)
        return absorb(n, slot, state, False)

    state = (jnp.full((1, tq), NEG, jnp.float32), jnp.zeros((1, tq), jnp.float32),
             jnp.zeros((head_dim, tq), jnp.float32))
    state = lax.fori_loop(0, n_masked, masked_step, state)

    @pl.when(full_hi > full_lo)
    def _():
        scores(full_lo, 0)

    m, l, acc = lax.fori_loop(full_lo, full_hi, full_step, state)
    o_ref[...] = (acc / l).T.astype(o_ref.dtype)


def attention(qkv, seg, heads, head_dim, tq, tk):
    length = qkv.shape[0]
    n_q = length // tq
    first, last = seg[::tq], seg[tq - 1::tq]
    start = jnp.sum(seg[None, :] < first[:, None], axis=1)
    stop = jnp.sum(seg[None, :] <= last[:, None], axis=1)
    lo, hi = start // tk, (stop + tk - 1) // tk
    full_lo, full_hi = (start + tk - 1) // tk, stop // tk
    plain = (first == last) & (full_hi > full_lo)
    full_lo = jnp.where(plain, full_lo, hi)
    full_hi = jnp.where(plain, full_hi, hi)
    bounds = jnp.stack([lo, full_lo, full_hi, hi]).astype(jnp.int32)
    segq = jnp.broadcast_to(seg[None, :], (8, length))
    segk = jnp.broadcast_to(seg[:, None], (length, 128))
    scale2 = head_dim ** -0.5 * math.log2(math.e)
    return pl.pallas_call(
        functools.partial(attention_kernel, tk, scale2),
        out_shape=jax.ShapeDtypeStruct((length, heads * head_dim), jnp.bfloat16),
        grid_spec=pltpu.PrefetchScalarGridSpec(
            num_scalar_prefetch=1, grid=(heads, n_q),
            in_specs=[
                pl.BlockSpec((tq, head_dim), lambda h, i, b: (i, h)),
                pl.BlockSpec((length, head_dim), lambda h, i, b: (0, heads + h)),
                pl.BlockSpec((length, head_dim), lambda h, i, b: (0, 2 * heads + h)),
                pl.BlockSpec((8, tq), lambda h, i, b: (0, i)),
                pl.BlockSpec((length, 128), lambda h, i, b: (0, 0)),
            ],
            out_specs=pl.BlockSpec((tq, head_dim), lambda h, i, b: (i, h)),
            scratch_shapes=[
                pltpu.VMEM((head_dim, length), jnp.bfloat16),
                pltpu.VMEM((2, tk, tq), jnp.float32),
            ]),
        compiler_params=pltpu.CompilerParams(vmem_limit_bytes=48 * 2**20),
        name='attention',
    )(bounds, qkv, qkv, qkv, segq, segk)


def solution(mesh):
    n_cp, n_sp = mesh.shape['cp'], mesh.shape['sp']
    n_blocks = n_cp * n_sp
    columns = n_cp // CORES
    token_spec = P('dp', ('cp', 'sp'), None)
    seg_spec = P('dp', ('cp', 'sp'))

    def local_layer(hidden, seg_ids, w_qkv, w_out):
        batch, tokens, depth = hidden.shape
        n_heads, head_dim = w_out.shape[:2]
        groups = n_blocks // batch
        assert n_sp == 4 and columns == 4 and groups == 4 and batch == 2 * columns
        heads = n_heads // groups
        x, core, pair, end = place(lax.axis_index('cp'), lax.axis_index('sp'))
        group = core * 2 + end
        seq = x * 2 + pair
        w_local = lax.dynamic_slice(w_qkv, (0, 0, group * heads, 0), (depth, 3, heads, head_dim))
        w_local = w_local.reshape(depth, 3 * heads * head_dim)
        qkv = gather_project(hidden, w_local, columns, n_blocks)

        seg = lax.all_gather(seg_ids, ('cp', 'sp'), axis=1, tiled=True)
        seg = lax.dynamic_slice(seg, (seq, 0), (1, tokens * n_blocks))[0]
        o = attention(qkv, seg, heads, head_dim, 512, 512)

        o = o.reshape(n_blocks, tokens, heads * head_dim)
        o = lax.all_to_all(o, ('cp', 'sp'), 0, 0, tiled=True)
        o = o.reshape(columns, CORES, 2, 2, tokens, heads * head_dim)
        o = o.transpose(0, 2, 4, 1, 3, 5).reshape(batch, tokens, n_heads * head_dim)
        y = jnp.dot(o, w_out.reshape(n_heads * head_dim, depth), preferred_element_type=jnp.float32)
        return y.astype(jnp.bfloat16)

    return jax.shard_map(local_layer, mesh=mesh, in_specs=(token_spec, seg_spec, P(), P()), out_specs=token_spec,
                         check_vma=False)
```

```python
import functools
import math

import jax
import jax.numpy as jnp
from jax import lax
from jax.experimental import pallas as pl
from jax.experimental.pallas import tpu as pltpu
from jax.sharding import PartitionSpec as P

MESH = pl.DeviceIdType.MESH
CORES = 2


def place(rank, lane):
    return rank // CORES, rank % CORES, lane // 2, lane % 2


def gather_project_kernel(columns, heads, hid, seg, w_hbm, out, seg_out, blocks, w_vmem, stage, w_in, w_wide, recv_sem,
                          direct_sem, relay_sem, twin_sem, w_sem, own_sem, out_sem, seg_send, seg_recv):
    rank, lane = lax.axis_index('cp'), lax.axis_index('sp')
    x, core, pair, end = place(rank, lane)
    far = 3 - lane
    mate = 2 * pair + 1 - end
    n_blocks = blocks.shape[0]
    lanes = n_blocks // (columns * CORES)

    def dev(xx, cc, yy):
        return {'cp': xx * CORES + cc, 'sp': yy}

    def slot_of(xx, hh, cc, ee):
        return ((xx * 2 + hh) * CORES + cc) * 2 + ee

    me = slot_of(x, pair, core, end)
    steps = [(dx, other) for dx in (0, 1, columns - 1, 2) for other in (0, 1)]
    n_groups = len(steps)
    twin = dev(x, 1 - core, lane)
    partner = dev(x, core, mate)

    def peer(k):
        p = (rank * lanes + lane + k) % n_blocks
        return {'cp': p // lanes, 'sp': p % lanes}

    barrier = pltpu.get_barrier_semaphore()

    def greet(k, carry):
        pl.semaphore_signal(barrier, inc=1, device_id=peer(k), device_id_type=MESH)
        return carry

    lax.fori_loop(1, n_blocks, greet, 0)

    own = pltpu.make_async_copy(hid.at[x * 2 + pair], blocks.at[me], own_sem.at[0])
    own.start()
    here = rank * lanes + lane
    own_seg = pltpu.make_async_copy(seg, seg_out.at[here], own_sem.at[1])
    own_seg.start()

    first = (core * 2 + end) * heads
    tile0 = jnp.minimum(first // 8, w_hbm.shape[2] // 8 - 2) * 8
    shift = first - tile0
    depth, width = w_vmem.shape
    chunk = w_in.shape[1]

    def w_copy(n):
        return pltpu.make_async_copy(
            w_hbm.at[pl.ds(pl.multiple_of(n * chunk, chunk), chunk), :, pl.ds(pl.multiple_of(tile0, 8), 16), :],
            w_in.at[n % 2], w_sem.at[n % 2])

    w_copy(0).start()
    pl.semaphore_wait(barrier, n_blocks - 1)

    directs = []
    for i, (dx, other) in enumerate(steps[1:]):
        xt = (x + columns - dx) % columns
        copy = pltpu.make_async_remote_copy(
            src_ref=hid.at[xt * 2 + (1 - pair if other else pair)], dst_ref=blocks.at[me], send_sem=direct_sem.at[i],
            recv_sem=recv_sem.at[me], device_id=dev(xt, core, far if other else lane), device_id_type=MESH)
        copy.start()
        directs.append(copy)

    def remote(slot, sem, device):
        return pltpu.make_async_remote_copy(
            src_ref=blocks.at[slot], dst_ref=blocks.at[slot], send_sem=sem, recv_sem=recv_sem.at[slot],
            device_id=device, device_id_type=MESH)

    def group(j):
        s = j // 2
        dx = s + jnp.where(s == 2, 1, 0) - jnp.where(s == 3, 1, 0)
        return (x + dx) % columns, (pair + j % 2) % 2

    def sides(j):
        de = jnp.where(j % 2 == 0, end, 1 - end)
        return de, 1 - de

    def serve(j):
        xs, hs = group(j)
        slot = slot_of(xs, hs, core, sides(j)[0])

        @pl.when(j > 0)
        def _():
            remote(slot, relay_sem.at[j], partner).wait_recv()

        remote(slot, relay_sem.at[j], partner).start()
        remote(slot, twin_sem.at[j, 0], twin).start()

    own.wait()
    serve(0)

    def send_seg(k, carry):
        pltpu.make_async_remote_copy(src_ref=seg, dst_ref=seg_out.at[here], send_sem=seg_send, recv_sem=seg_recv,
                                     device_id=peer(k), device_id_type=MESH).start()
        return carry

    lax.fori_loop(1, n_blocks, send_seg, 0)

    n_chunks = depth // chunk
    lane_width = w_wide.shape[1]

    def relay_weights(n, carry):
        @pl.when(n + 1 < n_chunks)
        def _():
            w_copy(n + 1).start()

        w_copy(n).wait()
        half = chunk * 8
        for kind in range(3):
            both = w_in[n % 2, :, kind].astype(jnp.float32)
            for part in range(2):
                w_wide[pl.ds((2 * kind + part) * half, half), :] = both[:, part * 8:part * 8 + 8].reshape(half, lane_width)
        for kind in range(3):
            for h in range(heads):
                row = (2 * kind + (shift + h) // 8) * half + (shift + h) % 8
                at = (kind * heads + h) * lane_width
                w_vmem[pl.ds(pl.multiple_of(n * chunk, chunk), chunk), pl.ds(at, lane_width)] = (
                    w_wide[pl.ds(row, chunk, stride=8), :].astype(jnp.bfloat16))
        return carry

    lax.fori_loop(0, n_chunks // 2, relay_weights, 0)
    serve(1)
    lax.fori_loop(n_chunks // 2, n_chunks, relay_weights, 0)

    rows = stage.shape[1] // 4
    tile = 256

    def out_copies(j):
        xs, hs = group(j)
        buf = j % 2
        return [pltpu.make_async_copy(
            stage.at[buf, pl.ds(k * rows, rows)],
            out.at[pl.ds(pl.multiple_of(((xs * CORES + k // 2) * lanes + hs * 2 + k % 2) * rows, rows), rows)],
            out_sem.at[buf, k]) for k in range(4)]

    def step(j, carry):
        xs, hs = group(j)
        de, ve = sides(j)

        @pl.when(j + 2 < n_groups)
        def _():
            serve(j + 2)

        via = slot_of(xs, hs, core, ve)
        remote(via, twin_sem.at[j, 1], twin).wait_recv()
        remote(via, twin_sem.at[j, 1], twin).start()
        remote(slot_of(xs, hs, 1 - core, de), twin_sem.at[j, 0], twin).wait_recv()
        remote(slot_of(xs, hs, 1 - core, ve), twin_sem.at[j, 1], twin).wait_recv()

        @pl.when(j >= 2)
        def _():
            for copy in out_copies(j - 2):
                copy.wait()

        lhs = blocks.at[pl.ds(slot_of(xs, hs, 0, 0), 4)]
        buf = j % 2

        def column(n, carry):
            c = pl.ds(pl.multiple_of(n * tile, tile), tile)
            acc = jnp.dot(lhs[...].reshape(4 * rows, depth), w_vmem[:, c], preferred_element_type=jnp.float32)
            stage[buf, :, c] = acc.astype(jnp.bfloat16)
            return carry

        lax.fori_loop(0, width // tile, column, 0)
        for copy in out_copies(j):
            copy.start()
        return carry

    lax.fori_loop(0, n_groups, step, 0)

    for copy in directs:
        copy.wait_send()

    def drain(j, carry):
        remote(me, relay_sem.at[j], partner).wait_send()
        remote(me, twin_sem.at[j, 0], twin).wait_send()
        remote(me, twin_sem.at[j, 1], twin).wait_send()

        @pl.when(j >= n_groups - 2)
        def _():
            for copy in out_copies(j):
                copy.wait()

        return carry

    lax.fori_loop(0, n_groups, drain, 0)
    others = seg_out.at[pl.ds(0, n_blocks - 1)]
    all_segs = pltpu.make_async_remote_copy(src_ref=others, dst_ref=others, send_sem=seg_send, recv_sem=seg_recv,
                                            device_id=twin, device_id_type=MESH)
    all_segs.wait_send()
    all_segs.wait_recv()
    own_seg.wait()


def gather_project(hidden, seg_ids, w_qkv, heads, columns, n_blocks):
    batch, tokens, depth = hidden.shape
    head_dim = w_qkv.shape[3]
    width = 3 * heads * head_dim
    n_groups = n_blocks // 4
    chunk = 64 if depth % 128 == 0 else depth
    return pl.pallas_call(
        functools.partial(gather_project_kernel, columns, heads),
        out_shape=(jax.ShapeDtypeStruct((n_blocks * tokens, width), jnp.bfloat16),
                   jax.ShapeDtypeStruct((n_blocks,) + seg_ids.shape, seg_ids.dtype)),
        in_specs=[pl.BlockSpec(memory_space=pl.ANY)] * 3,
        out_specs=[pl.BlockSpec(memory_space=pl.ANY)] * 2,
        scratch_shapes=[
            pltpu.VMEM((n_blocks, tokens, depth), jnp.bfloat16),
            pltpu.VMEM((depth, width), jnp.bfloat16),
            pltpu.VMEM((2, 4 * tokens, width), jnp.bfloat16),
            pltpu.VMEM((2, chunk, 3, 16, head_dim), jnp.bfloat16),
            pltpu.VMEM((3 * 16 * chunk, head_dim), jnp.float32),
            pltpu.SemaphoreType.DMA((n_blocks,)),
            pltpu.SemaphoreType.DMA((n_groups - 1,)),
            pltpu.SemaphoreType.DMA((n_groups,)),
            pltpu.SemaphoreType.DMA((n_groups, 2)),
            pltpu.SemaphoreType.DMA((2,)),
            pltpu.SemaphoreType.DMA((2,)),
            pltpu.SemaphoreType.DMA((2, 4)),
            pltpu.SemaphoreType.DMA,
            pltpu.SemaphoreType.DMA,
        ],
        compiler_params=pltpu.CompilerParams(collective_id=0, has_side_effects=True, vmem_limit_bytes=60 * 2**20),
        name='gather_project',
    )(hidden, seg_ids, w_qkv)


def attention_kernel(tk, scale2, bounds, q_ref, k_ref, v_ref, segq_ref, segk_ref, o_ref, vt, s_even, s_odd, acc):
    i = pl.program_id(1)
    tq, head_dim = q_ref.shape

    @pl.when(i == 0)
    def _():
        vt[...] = v_ref[...].T

    lo, hi = bounds[0, i], bounds[1, i]
    q = q_ref[...]

    def at(chunk):
        return pl.ds(pl.multiple_of(chunk * tk, tk), tk)

    def scores(chunk, s_ref):
        s = lax.dot_general(k_ref[at(chunk), :], q, (((1,), (1,)), ((), ())), preferred_element_type=jnp.float32)
        segk = segk_ref[at(chunk), :]
        allowed = jnp.concatenate([segk] * (tq // segk.shape[1]), axis=1) == segq_ref[:1, :]
        s = jnp.where(allowed, s, -jnp.inf)
        s_ref[...] = s
        return jnp.max(s, axis=0, keepdims=True)

    def absorb(chunk, s, top, m, l):
        m_new = jnp.maximum(m, top)
        p = jnp.exp2((s - m_new) * scale2)
        alpha = jnp.exp2((m - m_new) * scale2)
        l = l * alpha + jnp.sum(p, axis=0, keepdims=True)
        acc[...] = acc[...] * alpha + lax.dot_general(vt[:, at(chunk)], p.astype(jnp.bfloat16), (((1,), (0,)), ((), ())),
                                                      preferred_element_type=jnp.float32)
        return m_new, l

    def pair_step(n, state):
        m, l, top_even = state
        chunk = lo + 2 * n
        top_odd = scores(chunk + 1, s_odd)
        m, l = absorb(chunk, s_even[...], top_even, m, l)
        top_even = scores(jnp.minimum(chunk + 2, hi - 1), s_even)
        m, l = absorb(chunk + 1, s_odd[...], top_odd, m, l)
        return m, l, top_even

    acc[...] = jnp.zeros_like(acc)
    m, l = jnp.full((1, tq), jnp.finfo(jnp.float32).min, jnp.float32), jnp.zeros((1, tq), jnp.float32)
    top = scores(lo, s_even)
    m, l, top = lax.fori_loop(0, (hi - lo) // 2, pair_step, (m, l, top))
    m, l = lax.fori_loop(0, (hi - lo) % 2, lambda n, state: absorb(hi - 1, s_even[...], top, *state), (m, l))
    o_ref[...] = (acc[...] / l).T.astype(o_ref.dtype)


def attention(qkv, seg, heads, head_dim, tq, tk):
    length = qkv.shape[0]
    n_q = length // tq
    first, last = seg[::tq], seg[tq - 1::tq]
    start = jnp.sum(seg[None, :] < first[:, None], axis=1)
    stop = jnp.sum(seg[None, :] <= last[:, None], axis=1)
    bounds = jnp.stack([start // tk, (stop + tk - 1) // tk]).astype(jnp.int32)
    segq = jnp.broadcast_to(seg[None, :], (8, length))
    segk = jnp.broadcast_to(seg[:, None], (length, 128))
    scale2 = head_dim ** -0.5 * math.log2(math.e)
    return pl.pallas_call(
        functools.partial(attention_kernel, tk, scale2),
        out_shape=jax.ShapeDtypeStruct((length, heads * head_dim), jnp.bfloat16),
        grid_spec=pltpu.PrefetchScalarGridSpec(
            num_scalar_prefetch=1, grid=(heads, n_q),
            in_specs=[
                pl.BlockSpec((tq, head_dim), lambda h, i, b: (i, h)),
                pl.BlockSpec((length, head_dim), lambda h, i, b: (0, heads + h)),
                pl.BlockSpec((length, head_dim), lambda h, i, b: (0, 2 * heads + h)),
                pl.BlockSpec((8, tq), lambda h, i, b: (0, i)),
                pl.BlockSpec((length, 128), lambda h, i, b: (0, 0)),
            ],
            out_specs=pl.BlockSpec((tq, head_dim), lambda h, i, b: (i, h)),
            scratch_shapes=[
                pltpu.VMEM((head_dim, length), jnp.bfloat16),
                pltpu.VMEM((tk, tq), jnp.float32),
                pltpu.VMEM((tk, tq), jnp.float32),
                pltpu.VMEM((head_dim, tq), jnp.float32),
            ]),
        compiler_params=pltpu.CompilerParams(vmem_limit_bytes=48 * 2**20),
        name='attention',
    )(bounds, qkv, qkv, qkv, segq, segk)


def solution(mesh):
    n_cp, n_sp = mesh.shape['cp'], mesh.shape['sp']
    n_blocks = n_cp * n_sp
    columns = n_cp // CORES
    token_spec = P('dp', ('cp', 'sp'), None)
    seg_spec = P('dp', ('cp', 'sp'))

    def local_layer(hidden, seg_ids, w_qkv, w_out):
        batch, tokens, depth = hidden.shape
        n_heads, head_dim = w_out.shape[:2]
        groups = n_blocks // batch
        assert n_sp == 4 and columns == 4 and groups == 4 and batch == 2 * columns
        heads = n_heads // groups
        x, core, pair, end = place(lax.axis_index('cp'), lax.axis_index('sp'))
        seq = x * 2 + pair
        qkv, seg = gather_project(hidden, seg_ids, w_qkv, heads, columns, n_blocks)
        seg = lax.dynamic_slice(seg, (0, seq, 0), (n_blocks, 1, tokens)).reshape(n_blocks * tokens)
        o = attention(qkv, seg, heads, head_dim, 512, 512)

        o = o.reshape(n_blocks, tokens, heads * head_dim)
        o = lax.all_to_all(o, ('cp', 'sp'), 0, 0, tiled=True)
        o = o.reshape(columns, CORES, 2, 2, tokens, heads * head_dim)
        o = o.transpose(0, 2, 4, 1, 3, 5).reshape(batch, tokens, n_heads * head_dim)
        y = jnp.dot(o, w_out.reshape(n_heads * head_dim, depth), preferred_element_type=jnp.float32)
        return y.astype(jnp.bfloat16)

    return jax.shard_map(local_layer, mesh=mesh, in_specs=(token_spec, seg_spec, P(), P()), out_specs=token_spec,
                         check_vma=False)
```

```python
import functools
import math

import jax
import jax.numpy as jnp
from jax import lax
from jax.experimental import pallas as pl
from jax.experimental.pallas import tpu as pltpu
from jax.sharding import PartitionSpec as P

MESH = pl.DeviceIdType.MESH
CORES = 2
VMEM_LIMIT = 67043328


def place(rank, lane):
    return rank // CORES, rank % CORES, lane // 2, lane % 2


def gather_project_kernel(columns, heads, hid, seg, w_hbm, out, seg_out, blocks, w_vmem, stage, w_in, w_wide, recv_sem,
                          direct_sem, relay_sem, twin_sem, w_sem, own_sem, out_sem, seg_send, seg_recv):
    rank, lane = lax.axis_index('cp'), lax.axis_index('sp')
    x, core, pair, end = place(rank, lane)
    far = 3 - lane
    mate = 2 * pair + 1 - end
    n_blocks = blocks.shape[0]
    lanes = n_blocks // (columns * CORES)

    def dev(xx, cc, yy):
        return {'cp': xx * CORES + cc, 'sp': yy}

    def slot_of(xx, hh, cc, ee):
        return ((xx * 2 + hh) * CORES + cc) * 2 + ee

    me = slot_of(x, pair, core, end)
    steps = [(dx, other) for dx in (0, 1, columns - 1, 2) for other in (0, 1)]
    n_groups = len(steps)
    twin = dev(x, 1 - core, lane)
    partner = dev(x, core, mate)

    def peer(k):
        p = (rank * lanes + lane + k) % n_blocks
        return {'cp': p // lanes, 'sp': p % lanes}

    barrier = pltpu.get_barrier_semaphore()

    def greet(k, carry):
        pl.semaphore_signal(barrier, inc=1, device_id=peer(k), device_id_type=MESH)
        return carry

    lax.fori_loop(1, n_blocks, greet, 0)

    own = pltpu.make_async_copy(hid.at[x * 2 + pair], blocks.at[me], own_sem.at[0])
    own.start()
    here = rank * lanes + lane
    own_seg = pltpu.make_async_copy(seg, seg_out.at[here], own_sem.at[1])
    own_seg.start()

    first = (core * 2 + end) * heads
    tile0 = jnp.minimum(first // 8, w_hbm.shape[2] // 8 - 2) * 8
    shift = first - tile0
    depth, width = w_vmem.shape
    chunk = w_in.shape[1]

    def w_copy(n):
        return pltpu.make_async_copy(
            w_hbm.at[pl.ds(pl.multiple_of(n * chunk, chunk), chunk), :, pl.ds(pl.multiple_of(tile0, 8), 16), :],
            w_in.at[n % 2], w_sem.at[n % 2])

    w_copy(0).start()
    pl.semaphore_wait(barrier, n_blocks - 1)

    directs = []
    for i, (dx, other) in enumerate(steps[1:]):
        xt = (x + columns - dx) % columns
        copy = pltpu.make_async_remote_copy(
            src_ref=hid.at[xt * 2 + (1 - pair if other else pair)], dst_ref=blocks.at[me], send_sem=direct_sem.at[i],
            recv_sem=recv_sem.at[me], device_id=dev(xt, core, far if other else lane), device_id_type=MESH)
        copy.start()
        directs.append(copy)

    def remote(slot, sem, device):
        return pltpu.make_async_remote_copy(
            src_ref=blocks.at[slot], dst_ref=blocks.at[slot], send_sem=sem, recv_sem=recv_sem.at[slot],
            device_id=device, device_id_type=MESH)

    def group(j):
        s = j // 2
        dx = s + jnp.where(s == 2, 1, 0) - jnp.where(s == 3, 1, 0)
        return (x + dx) % columns, (pair + j % 2) % 2

    def sides(j):
        de = jnp.where(j % 2 == 0, end, 1 - end)
        return de, 1 - de

    def serve(j):
        xs, hs = group(j)
        slot = slot_of(xs, hs, core, sides(j)[0])

        @pl.when(j > 0)
        def _():
            remote(slot, relay_sem.at[j], partner).wait_recv()

        remote(slot, relay_sem.at[j], partner).start()
        remote(slot, twin_sem.at[j, 0], twin).start()

    own.wait()
    serve(0)

    def send_seg(k, carry):
        pltpu.make_async_remote_copy(src_ref=seg, dst_ref=seg_out.at[here], send_sem=seg_send, recv_sem=seg_recv,
                                     device_id=peer(k), device_id_type=MESH).start()
        return carry

    lax.fori_loop(1, n_blocks, send_seg, 0)

    n_chunks = depth // chunk
    lane_width = w_wide.shape[1]

    def relay_weights(n, carry):
        @pl.when(n + 1 < n_chunks)
        def _():
            w_copy(n + 1).start()

        w_copy(n).wait()
        half = chunk * 8
        for kind in range(3):
            both = w_in[n % 2, :, kind].astype(jnp.float32)
            for part in range(2):
                w_wide[pl.ds((2 * kind + part) * half, half), :] = both[:, part * 8:part * 8 + 8].reshape(half, lane_width)
        for kind in range(3):
            for h in range(heads):
                row = (2 * kind + (shift + h) // 8) * half + (shift + h) % 8
                at = (kind * heads + h) * lane_width
                w_vmem[pl.ds(pl.multiple_of(n * chunk, chunk), chunk), pl.ds(at, lane_width)] = (
                    w_wide[pl.ds(row, chunk, stride=8), :].astype(jnp.bfloat16))
        return carry

    lax.fori_loop(0, n_chunks // 2, relay_weights, 0)
    serve(1)
    lax.fori_loop(n_chunks // 2, n_chunks, relay_weights, 0)

    rows = stage.shape[1] // 4
    tile = 256

    def out_copies(j):
        xs, hs = group(j)
        buf = j % 2
        return [pltpu.make_async_copy(
            stage.at[buf, pl.ds(k * rows, rows)],
            out.at[pl.ds(pl.multiple_of(((xs * CORES + k // 2) * lanes + hs * 2 + k % 2) * rows, rows), rows)],
            out_sem.at[buf, k]) for k in range(4)]

    def step(j, carry):
        xs, hs = group(j)
        de, ve = sides(j)

        @pl.when(j + 2 < n_groups)
        def _():
            serve(j + 2)

        via = slot_of(xs, hs, core, ve)
        remote(via, twin_sem.at[j, 1], twin).wait_recv()
        remote(via, twin_sem.at[j, 1], twin).start()
        remote(slot_of(xs, hs, 1 - core, de), twin_sem.at[j, 0], twin).wait_recv()
        remote(slot_of(xs, hs, 1 - core, ve), twin_sem.at[j, 1], twin).wait_recv()

        @pl.when(j >= 2)
        def _():
            for copy in out_copies(j - 2):
                copy.wait()

        lhs = blocks.at[pl.ds(slot_of(xs, hs, 0, 0), 4)]
        buf = j % 2

        def column(n, carry):
            c = pl.ds(pl.multiple_of(n * tile, tile), tile)
            acc = jnp.dot(lhs[...].reshape(4 * rows, depth), w_vmem[:, c], preferred_element_type=jnp.float32)
            stage[buf, :, c] = acc.astype(jnp.bfloat16)
            return carry

        lax.fori_loop(0, width // tile, column, 0)
        for copy in out_copies(j):
            copy.start()
        return carry

    lax.fori_loop(0, n_groups, step, 0)

    for copy in directs:
        copy.wait_send()

    def drain(j, carry):
        remote(me, relay_sem.at[j], partner).wait_send()
        remote(me, twin_sem.at[j, 0], twin).wait_send()
        remote(me, twin_sem.at[j, 1], twin).wait_send()

        @pl.when(j >= n_groups - 2)
        def _():
            for copy in out_copies(j):
                copy.wait()

        return carry

    lax.fori_loop(0, n_groups, drain, 0)
    others = seg_out.at[pl.ds(0, n_blocks - 1)]
    all_segs = pltpu.make_async_remote_copy(src_ref=others, dst_ref=others, send_sem=seg_send, recv_sem=seg_recv,
                                            device_id=twin, device_id_type=MESH)
    all_segs.wait_send()
    all_segs.wait_recv()
    own_seg.wait()


def gather_project(hidden, seg_ids, w_qkv, heads, columns, n_blocks):
    batch, tokens, depth = hidden.shape
    head_dim = w_qkv.shape[3]
    width = 3 * heads * head_dim
    n_groups = n_blocks // 4
    chunk = 64 if depth % 128 == 0 else depth
    return pl.pallas_call(
        functools.partial(gather_project_kernel, columns, heads),
        out_shape=(jax.ShapeDtypeStruct((n_blocks * tokens, width), jnp.bfloat16),
                   jax.ShapeDtypeStruct((n_blocks,) + seg_ids.shape, seg_ids.dtype)),
        in_specs=[pl.BlockSpec(memory_space=pl.ANY)] * 3,
        out_specs=[pl.BlockSpec(memory_space=pl.ANY)] * 2,
        scratch_shapes=[
            pltpu.VMEM((n_blocks, tokens, depth), jnp.bfloat16),
            pltpu.VMEM((depth, width), jnp.bfloat16),
            pltpu.VMEM((2, 4 * tokens, width), jnp.bfloat16),
            pltpu.VMEM((2, chunk, 3, 16, head_dim), jnp.bfloat16),
            pltpu.VMEM((3 * 16 * chunk, head_dim), jnp.float32),
            pltpu.SemaphoreType.DMA((n_blocks,)),
            pltpu.SemaphoreType.DMA((n_groups - 1,)),
            pltpu.SemaphoreType.DMA((n_groups,)),
            pltpu.SemaphoreType.DMA((n_groups, 2)),
            pltpu.SemaphoreType.DMA((2,)),
            pltpu.SemaphoreType.DMA((2,)),
            pltpu.SemaphoreType.DMA((2, 4)),
            pltpu.SemaphoreType.DMA,
            pltpu.SemaphoreType.DMA,
        ],
        compiler_params=pltpu.CompilerParams(collective_id=0, has_side_effects=True, vmem_limit_bytes=VMEM_LIMIT),
        name='gather_project',
    )(hidden, seg_ids, w_qkv)


def attention_kernel(tk, scale2, bounds, q_ref, k_ref, v_ref, segq_ref, segk_ref, o_ref, vt, s_even, s_odd, acc):
    i = pl.program_id(1)
    tq, head_dim = q_ref.shape

    @pl.when(i == 0)
    def _():
        vt[...] = v_ref[...].T

    lo, hi = bounds[0, i], bounds[1, i]
    q = q_ref[...]

    def at(chunk):
        return pl.ds(pl.multiple_of(chunk * tk, tk), tk)

    def scores(chunk, s_ref):
        s = lax.dot_general(k_ref[at(chunk), :], q, (((1,), (1,)), ((), ())), preferred_element_type=jnp.float32)
        segk = segk_ref[at(chunk), :]
        allowed = jnp.concatenate([segk] * (tq // segk.shape[1]), axis=1) == segq_ref[:1, :]
        s = jnp.where(allowed, s, -jnp.inf)
        s_ref[...] = s
        return jnp.max(s, axis=0, keepdims=True)

    def absorb(chunk, s, top, m, l):
        m_new = jnp.maximum(m, top)
        p = jnp.exp2((s - m_new) * scale2)
        alpha = jnp.exp2((m - m_new) * scale2)
        l = l * alpha + jnp.sum(p, axis=0, keepdims=True)
        acc[...] = acc[...] * alpha + lax.dot_general(vt[:, at(chunk)], p.astype(jnp.bfloat16), (((1,), (0,)), ((), ())),
                                                      preferred_element_type=jnp.float32)
        return m_new, l

    def pair_step(n, state):
        m, l, top_even = state
        chunk = lo + 2 * n
        top_odd = scores(chunk + 1, s_odd)
        m, l = absorb(chunk, s_even[...], top_even, m, l)
        top_even = scores(jnp.minimum(chunk + 2, hi - 1), s_even)
        m, l = absorb(chunk + 1, s_odd[...], top_odd, m, l)
        return m, l, top_even

    acc[...] = jnp.zeros_like(acc)
    m, l = jnp.full((1, tq), jnp.finfo(jnp.float32).min, jnp.float32), jnp.zeros((1, tq), jnp.float32)
    top = scores(lo, s_even)
    m, l, top = lax.fori_loop(0, (hi - lo) // 2, pair_step, (m, l, top))
    m, l = lax.fori_loop(0, (hi - lo) % 2, lambda n, state: absorb(hi - 1, s_even[...], top, *state), (m, l))
    o_ref[...] = (acc[...] / l).T.astype(o_ref.dtype)


def attention(qkv, seg, heads, head_dim, tq, tk, h0, nh):
    length = qkv.shape[0]
    n_q = length // tq
    first, last = seg[::tq], seg[tq - 1::tq]
    start = jnp.sum(seg[None, :] < first[:, None], axis=1)
    stop = jnp.sum(seg[None, :] <= last[:, None], axis=1)
    bounds = jnp.stack([start // tk, (stop + tk - 1) // tk]).astype(jnp.int32)
    segq = jnp.broadcast_to(seg[None, :], (8, length))
    segk = jnp.broadcast_to(seg[:, None], (length, 128))
    scale2 = head_dim ** -0.5 * math.log2(math.e)
    return pl.pallas_call(
        functools.partial(attention_kernel, tk, scale2),
        out_shape=jax.ShapeDtypeStruct((length, nh * head_dim), jnp.bfloat16),
        grid_spec=pltpu.PrefetchScalarGridSpec(
            num_scalar_prefetch=1, grid=(nh, n_q),
            in_specs=[
                pl.BlockSpec((tq, head_dim), lambda h, i, b: (i, h0 + h)),
                pl.BlockSpec((length, head_dim), lambda h, i, b: (0, heads + h0 + h)),
                pl.BlockSpec((length, head_dim), lambda h, i, b: (0, 2 * heads + h0 + h)),
                pl.BlockSpec((8, tq), lambda h, i, b: (0, i)),
                pl.BlockSpec((length, 128), lambda h, i, b: (0, 0)),
            ],
            out_specs=pl.BlockSpec((tq, head_dim), lambda h, i, b: (i, h)),
            scratch_shapes=[
                pltpu.VMEM((head_dim, length), jnp.bfloat16),
                pltpu.VMEM((tk, tq), jnp.float32),
                pltpu.VMEM((tk, tq), jnp.float32),
                pltpu.VMEM((head_dim, tq), jnp.float32),
            ]),
        compiler_params=pltpu.CompilerParams(vmem_limit_bytes=VMEM_LIMIT),
        cost_estimate=pl.CostEstimate(flops=4 * nh * length * length * head_dim, transcendentals=0,
                                      bytes_accessed=8 * nh * length * head_dim),
        name='attention',
    )(bounds, qkv, qkv, qkv, segq, segk)


def out_kernel(columns, heads, parts, has_acc, *refs):
    n = len(parts)
    o_refs, w_ref, refs = refs[:n], refs[n], refs[n + 1:]
    acc_ref, refs = (refs[0], refs[1:]) if has_acc else (None, refs)
    y_ref, lhs, sem = refs
    batch, tokens = lhs.shape[:2]

    @pl.when(pl.program_id(0) == 0)
    def _():
        copies = []
        for seq in range(batch):
            at = 0
            for group in range(4):
                source = (seq // 2) * 8 + (group // 2) * 4 + (seq % 2) * 2 + group % 2
                for k in range(n):
                    size = o_refs[k].shape[2]
                    copies.append(pltpu.make_async_copy(o_refs[k].at[source], lhs.at[seq, :, pl.ds(at, size)], sem))
                    at += size
        for copy in copies:
            copy.start()
        for copy in copies:
            copy.wait()

    depth = lhs.shape[2]
    y = jnp.dot(lhs[...].reshape(batch * tokens, depth), w_ref[...].reshape(depth, w_ref.shape[-1]),
                preferred_element_type=jnp.float32)
    y = y.reshape(y_ref.shape)
    if has_acc:
        y = acc_ref[...] + y
    y_ref[...] = y.astype(y_ref.dtype)


def out_project(os, starts, w_out, acc, columns, heads, dtype, tile=256):
    n_heads, head_dim, width = w_out.shape
    n_blocks, tokens, _ = os[0].shape
    groups = n_heads // heads
    batch = n_blocks // groups
    count = sum(o.shape[2] for o in os) // head_dim
    first = starts[0]
    w = w_out.reshape(groups, heads, head_dim, width)
    w_spec = pl.BlockSpec(tuple(pl.Element(n) for n in (groups, count, head_dim, tile)), lambda i: (0, first, 0, i * tile))
    y_spec = pl.BlockSpec((batch, tokens, tile), lambda i: (0, 0, i))
    ins = [*os, w] + ([] if acc is None else [acc])
    return pl.pallas_call(
        functools.partial(out_kernel, columns, heads, starts, acc is not None),
        out_shape=jax.ShapeDtypeStruct((batch, tokens, width), dtype),
        grid=(width // tile,),
        in_specs=[pl.BlockSpec(memory_space=pl.ANY)] * len(os) + [w_spec] + ([] if acc is None else [y_spec]),
        out_specs=y_spec,
        scratch_shapes=[pltpu.VMEM((batch, tokens, groups * count * head_dim), jnp.bfloat16), pltpu.SemaphoreType.DMA],
        compiler_params=pltpu.CompilerParams(vmem_limit_bytes=VMEM_LIMIT),
        cost_estimate=pl.CostEstimate(flops=2 * batch * tokens * groups * count * head_dim * width, transcendentals=0,
                                      bytes_accessed=2 * groups * count * head_dim * width),
        name='out_project',
    )(*ins)


def solution(mesh):
    n_cp, n_sp = mesh.shape['cp'], mesh.shape['sp']
    n_blocks = n_cp * n_sp
    columns = n_cp // CORES
    token_spec = P('dp', ('cp', 'sp'), None)
    seg_spec = P('dp', ('cp', 'sp'))

    def local_layer(hidden, seg_ids, w_qkv, w_out):
        batch, tokens, depth = hidden.shape
        n_heads, head_dim = w_out.shape[:2]
        groups = n_blocks // batch
        assert n_sp == 4 and columns == 4 and groups == 4 and batch == 2 * columns
        heads = n_heads // groups
        x, core, pair, end = place(lax.axis_index('cp'), lax.axis_index('sp'))
        seq = x * 2 + pair
        qkv, seg = gather_project(hidden, seg_ids, w_qkv, heads, columns, n_blocks)
        seg = lax.dynamic_slice(seg, (0, seq, 0), (n_blocks, 1, tokens)).reshape(n_blocks * tokens)
        parts = ((0, heads // 3), (heads // 3, heads // 2), (heads - heads // 6, heads // 6))
        os = []
        for h0, nh in parts:
            o = attention(qkv, seg, heads, head_dim, 512, 512, h0, nh)
            o = o.reshape(n_blocks, tokens, nh * head_dim)
            os.append(lax.all_to_all(o, ('cp', 'sp'), 0, 0, tiled=True))
        starts = [h0 for h0, _ in parts]
        acc = out_project(os[:-1], starts[:-1], w_out, None, columns, heads, jnp.float32)
        return out_project(os[-1:], starts[-1:], w_out, acc, columns, heads, jnp.bfloat16)

    return jax.shard_map(local_layer, mesh=mesh, in_specs=(token_spec, seg_spec, P(), P()), out_specs=token_spec,
                         check_vma=False)
```

```python
import functools
import math

import jax
import jax.numpy as jnp
from jax import lax
from jax.experimental import pallas as pl
from jax.experimental.pallas import tpu as pltpu
from jax.sharding import PartitionSpec as P

MESH = pl.DeviceIdType.MESH
CORES = 2
VMEM_LIMIT = 67043328


def place(rank, lane):
    return rank // CORES, rank % CORES, lane // 2, lane % 2


def gather_project_kernel(columns, heads, hid, seg, w_hbm, out, seg_out, blocks, w_vmem, stage, w_in, w_wide, recv_sem,
                          direct_sem, relay_sem, twin_sem, w_sem, own_sem, out_sem, seg_send, seg_recv, transit, transit_recv,
                          transit_send):
    rank, lane = lax.axis_index('cp'), lax.axis_index('sp')
    x, core, pair, end = place(rank, lane)
    far = 3 - lane
    mate = 2 * pair + 1 - end
    n_blocks = blocks.shape[0]
    lanes = n_blocks // (columns * CORES)

    def dev(xx, cc, yy):
        return {'cp': xx * CORES + cc, 'sp': yy}

    def slot_of(xx, hh, cc, ee):
        return ((xx * 2 + hh) * CORES + cc) * 2 + ee

    me = slot_of(x, pair, core, end)
    n_groups = n_blocks // 4
    twin = dev(x, 1 - core, lane)
    partner = dev(x, core, mate)

    def peer(k):
        p = (rank * lanes + lane + k) % n_blocks
        return {'cp': p // lanes, 'sp': p % lanes}

    barrier = pltpu.get_barrier_semaphore()

    def greet(k, carry):
        pl.semaphore_signal(barrier, inc=1, device_id=peer(k), device_id_type=MESH)
        return carry

    lax.fori_loop(1, n_blocks, greet, 0)

    own = pltpu.make_async_copy(hid.at[x * 2 + pair], blocks.at[me], own_sem.at[0])
    own.start()
    here = rank * lanes + lane
    own_seg = pltpu.make_async_copy(seg, seg_out.at[here], own_sem.at[1])
    own_seg.start()

    first = (core * 2 + end) * heads
    tile0 = jnp.minimum(first // 8, w_hbm.shape[2] // 8 - 2) * 8
    shift = first - tile0
    depth, width = w_vmem.shape
    chunk = w_in.shape[1]

    def w_copy(n):
        return pltpu.make_async_copy(
            w_hbm.at[pl.ds(pl.multiple_of(n * chunk, chunk), chunk), :, pl.ds(pl.multiple_of(tile0, 8), 16), :],
            w_in.at[n % 2], w_sem.at[n % 2])

    w_copy(0).start()
    pl.semaphore_wait(barrier, n_blocks - 1)

    right, left = (x + 1) % columns, (x + columns - 1) % columns
    across = (x + 2) % columns
    directs = []
    sends = [(across * 2 + pair, transit.at[0], transit_recv.at[0], dev(right, core, lane)),
             (across * 2 + 1 - pair, transit.at[1], transit_recv.at[1], dev(left, core, lane))]
    for xt, other in ((x, 1), (left, 0), (right, 0), (left, 1), (right, 1)):
        sends.append((xt * 2 + (1 - pair if other else pair), blocks.at[me], recv_sem.at[me],
                      dev(xt, core, far if other else lane)))
    for i, (seq, place_, sem, device) in enumerate(sends):
        copy = pltpu.make_async_remote_copy(src_ref=hid.at[seq], dst_ref=place_, send_sem=direct_sem.at[i], recv_sem=sem,
                                            device_id=device, device_id_type=MESH)
        copy.start()
        directs.append(copy)

    passes = [
        pltpu.make_async_remote_copy(
            src_ref=transit.at[0], dst_ref=blocks.at[slot_of(left, pair, core, end)], send_sem=transit_send.at[0],
            recv_sem=recv_sem.at[slot_of(left, pair, core, end)], device_id=dev(right, core, lane), device_id_type=MESH),
        pltpu.make_async_remote_copy(
            src_ref=transit.at[1], dst_ref=blocks.at[slot_of(right, pair, core, end)], send_sem=transit_send.at[1],
            recv_sem=recv_sem.at[slot_of(right, pair, core, end)], device_id=dev(left, core, far), device_id_type=MESH)]
    arrivals = [pltpu.make_async_remote_copy(
        src_ref=transit.at[n], dst_ref=transit.at[n], send_sem=transit_send.at[n], recv_sem=transit_recv.at[n],
        device_id=twin, device_id_type=MESH) for n in range(2)]

    def remote(slot, sem, device):
        return pltpu.make_async_remote_copy(
            src_ref=blocks.at[slot], dst_ref=blocks.at[slot], send_sem=sem, recv_sem=recv_sem.at[slot],
            device_id=device, device_id_type=MESH)

    def group(j):
        s = j // 2
        dx = s + jnp.where(s == 2, 1, 0) - jnp.where(s == 3, 1, 0)
        return (x + dx) % columns, (pair + j % 2) % 2

    def sides(j):
        de = jnp.where(j % 2 == 0, end, 1 - end)
        return de, 1 - de

    def serve(j):
        xs, hs = group(j)
        slot = slot_of(xs, hs, core, sides(j)[0])

        @pl.when(j > 0)
        def _():
            remote(slot, relay_sem.at[j], partner).wait_recv()

        remote(slot, relay_sem.at[j], partner).start()
        remote(slot, twin_sem.at[j, 0], twin).start()

    own.wait()
    serve(0)

    def send_seg(k, carry):
        pltpu.make_async_remote_copy(src_ref=seg, dst_ref=seg_out.at[here], send_sem=seg_send, recv_sem=seg_recv,
                                     device_id=peer(k), device_id_type=MESH).start()
        return carry

    lax.fori_loop(1, n_blocks, send_seg, 0)

    n_chunks = depth // chunk
    lane_width = w_wide.shape[1]

    def relay_weights(n, carry):
        @pl.when(n + 1 < n_chunks)
        def _():
            w_copy(n + 1).start()

        w_copy(n).wait()
        half = chunk * 8
        for kind in range(3):
            both = w_in[n % 2, :, kind].astype(jnp.float32)
            for part in range(2):
                w_wide[pl.ds((2 * kind + part) * half, half), :] = both[:, part * 8:part * 8 + 8].reshape(half, lane_width)
        for kind in range(3):
            for h in range(heads):
                row = (2 * kind + (shift + h) // 8) * half + (shift + h) % 8
                at = (kind * heads + h) * lane_width
                w_vmem[pl.ds(pl.multiple_of(n * chunk, chunk), chunk), pl.ds(at, lane_width)] = (
                    w_wide[pl.ds(row, chunk, stride=8), :].astype(jnp.bfloat16))
        return carry

    lax.fori_loop(0, n_chunks // 2, relay_weights, 0)
    serve(1)
    lax.fori_loop(n_chunks // 2, n_chunks, relay_weights, 0)
    for arrival, copy in zip(arrivals, passes):
        arrival.wait_recv()
        copy.start()

    rows = stage.shape[1] // 4
    tile = 256

    def out_copies(j):
        xs, hs = group(j)
        buf = j % 2
        return [pltpu.make_async_copy(
            stage.at[buf, pl.ds(k * rows, rows)],
            out.at[pl.ds(pl.multiple_of(((xs * CORES + k // 2) * lanes + hs * 2 + k % 2) * rows, rows), rows)],
            out_sem.at[buf, k]) for k in range(4)]

    def step(j, carry):
        xs, hs = group(j)
        de, ve = sides(j)

        @pl.when(j + 2 < n_groups)
        def _():
            serve(j + 2)

        via = slot_of(xs, hs, core, ve)
        remote(via, twin_sem.at[j, 1], twin).wait_recv()
        remote(via, twin_sem.at[j, 1], twin).start()
        remote(slot_of(xs, hs, 1 - core, de), twin_sem.at[j, 0], twin).wait_recv()
        remote(slot_of(xs, hs, 1 - core, ve), twin_sem.at[j, 1], twin).wait_recv()

        @pl.when(j >= 2)
        def _():
            for copy in out_copies(j - 2):
                copy.wait()

        lhs = blocks.at[pl.ds(slot_of(xs, hs, 0, 0), 4)]
        buf = j % 2

        def column(n, carry):
            c = pl.ds(pl.multiple_of(n * tile, tile), tile)
            acc = jnp.dot(lhs[...].reshape(4 * rows, depth), w_vmem[:, c], preferred_element_type=jnp.float32)
            stage[buf, :, c] = acc.astype(jnp.bfloat16)
            return carry

        lax.fori_loop(0, width // tile, column, 0)
        for copy in out_copies(j):
            copy.start()
        return carry

    lax.fori_loop(0, n_groups, step, 0)

    for copy in directs + passes:
        copy.wait_send()

    def drain(j, carry):
        remote(me, relay_sem.at[j], partner).wait_send()
        remote(me, twin_sem.at[j, 0], twin).wait_send()
        remote(me, twin_sem.at[j, 1], twin).wait_send()

        @pl.when(j >= n_groups - 2)
        def _():
            for copy in out_copies(j):
                copy.wait()

        return carry

    lax.fori_loop(0, n_groups, drain, 0)
    others = seg_out.at[pl.ds(0, n_blocks - 1)]
    all_segs = pltpu.make_async_remote_copy(src_ref=others, dst_ref=others, send_sem=seg_send, recv_sem=seg_recv,
                                            device_id=twin, device_id_type=MESH)
    all_segs.wait_send()
    all_segs.wait_recv()
    own_seg.wait()


def gather_project(hidden, seg_ids, w_qkv, heads, columns, n_blocks):
    batch, tokens, depth = hidden.shape
    head_dim = w_qkv.shape[3]
    width = 3 * heads * head_dim
    n_groups = n_blocks // 4
    chunk = 64 if depth % 128 == 0 else depth
    return pl.pallas_call(
        functools.partial(gather_project_kernel, columns, heads),
        out_shape=(jax.ShapeDtypeStruct((n_blocks * tokens, width), jnp.bfloat16),
                   jax.ShapeDtypeStruct((n_blocks,) + seg_ids.shape, seg_ids.dtype)),
        in_specs=[pl.BlockSpec(memory_space=pl.ANY)] * 3,
        out_specs=[pl.BlockSpec(memory_space=pl.ANY)] * 2,
        scratch_shapes=[
            pltpu.VMEM((n_blocks, tokens, depth), jnp.bfloat16),
            pltpu.VMEM((depth, width), jnp.bfloat16),
            pltpu.VMEM((2, 4 * tokens, width), jnp.bfloat16),
            pltpu.VMEM((2, chunk, 3, 16, head_dim), jnp.bfloat16),
            pltpu.VMEM((3 * 16 * chunk, head_dim), jnp.float32),
            pltpu.SemaphoreType.DMA((n_blocks,)),
            pltpu.SemaphoreType.DMA((n_groups - 1,)),
            pltpu.SemaphoreType.DMA((n_groups,)),
            pltpu.SemaphoreType.DMA((n_groups, 2)),
            pltpu.SemaphoreType.DMA((2,)),
            pltpu.SemaphoreType.DMA((2,)),
            pltpu.SemaphoreType.DMA((2, 4)),
            pltpu.SemaphoreType.DMA,
            pltpu.SemaphoreType.DMA,
            pltpu.VMEM((2, tokens, depth), jnp.bfloat16),
            pltpu.SemaphoreType.DMA((2,)),
            pltpu.SemaphoreType.DMA((2,)),
        ],
        compiler_params=pltpu.CompilerParams(collective_id=0, has_side_effects=True, vmem_limit_bytes=VMEM_LIMIT),
        name='gather_project',
    )(hidden, seg_ids, w_qkv)


def attention_kernel(tk, scale2, bounds, q_ref, k_ref, v_ref, segq_ref, segk_ref, o_ref, vt, s_even, s_odd, acc):
    i = pl.program_id(1)
    tq, head_dim = q_ref.shape

    @pl.when(i == 0)
    def _():
        vt[...] = v_ref[...].T

    lo, hi = bounds[0, i], bounds[1, i]
    q = q_ref[...]

    def at(chunk):
        return pl.ds(pl.multiple_of(chunk * tk, tk), tk)

    def scores(chunk, s_ref):
        s = lax.dot_general(k_ref[at(chunk), :], q, (((1,), (1,)), ((), ())), preferred_element_type=jnp.float32)
        segk = segk_ref[at(chunk), :]
        allowed = jnp.concatenate([segk] * (tq // segk.shape[1]), axis=1) == segq_ref[:1, :]
        s = jnp.where(allowed, s, -jnp.inf)
        s_ref[...] = s
        return jnp.max(s, axis=0, keepdims=True)

    def absorb(chunk, s, top, m, l):
        m_new = jnp.maximum(m, top)
        p = jnp.exp2((s - m_new) * scale2)
        alpha = jnp.exp2((m - m_new) * scale2)
        l = l * alpha + jnp.sum(p, axis=0, keepdims=True)
        acc[...] = acc[...] * alpha + lax.dot_general(vt[:, at(chunk)], p.astype(jnp.bfloat16), (((1,), (0,)), ((), ())),
                                                      preferred_element_type=jnp.float32)
        return m_new, l

    def pair_step(n, state):
        m, l, top_even = state
        chunk = lo + 2 * n
        top_odd = scores(chunk + 1, s_odd)
        m, l = absorb(chunk, s_even[...], top_even, m, l)
        top_even = scores(jnp.minimum(chunk + 2, hi - 1), s_even)
        m, l = absorb(chunk + 1, s_odd[...], top_odd, m, l)
        return m, l, top_even

    acc[...] = jnp.zeros_like(acc)
    m, l = jnp.full((1, tq), jnp.finfo(jnp.float32).min, jnp.float32), jnp.zeros((1, tq), jnp.float32)
    top = scores(lo, s_even)
    m, l, top = lax.fori_loop(0, (hi - lo) // 2, pair_step, (m, l, top))
    m, l = lax.fori_loop(0, (hi - lo) % 2, lambda n, state: absorb(hi - 1, s_even[...], top, *state), (m, l))
    o_ref[...] = (acc[...] / l).T.astype(o_ref.dtype)


def attention(qkv, seg, heads, head_dim, tq, tk, h0, nh):
    length = qkv.shape[0]
    n_q = length // tq
    first, last = seg[::tq], seg[tq - 1::tq]
    start = jnp.sum(seg[None, :] < first[:, None], axis=1)
    stop = jnp.sum(seg[None, :] <= last[:, None], axis=1)
    bounds = jnp.stack([start // tk, (stop + tk - 1) // tk]).astype(jnp.int32)
    segq = jnp.broadcast_to(seg[None, :], (8, length))
    segk = jnp.broadcast_to(seg[:, None], (length, 128))
    scale2 = head_dim ** -0.5 * math.log2(math.e)
    return pl.pallas_call(
        functools.partial(attention_kernel, tk, scale2),
        out_shape=jax.ShapeDtypeStruct((length, nh * head_dim), jnp.bfloat16),
        grid_spec=pltpu.PrefetchScalarGridSpec(
            num_scalar_prefetch=1, grid=(nh, n_q),
            in_specs=[
                pl.BlockSpec((tq, head_dim), lambda h, i, b: (i, h0 + h)),
                pl.BlockSpec((length, head_dim), lambda h, i, b: (0, heads + h0 + h)),
                pl.BlockSpec((length, head_dim), lambda h, i, b: (0, 2 * heads + h0 + h)),
                pl.BlockSpec((8, tq), lambda h, i, b: (0, i)),
                pl.BlockSpec((length, 128), lambda h, i, b: (0, 0)),
            ],
            out_specs=pl.BlockSpec((tq, head_dim), lambda h, i, b: (i, h)),
            scratch_shapes=[
                pltpu.VMEM((head_dim, length), jnp.bfloat16),
                pltpu.VMEM((tk, tq), jnp.float32),
                pltpu.VMEM((tk, tq), jnp.float32),
                pltpu.VMEM((head_dim, tq), jnp.float32),
            ]),
        compiler_params=pltpu.CompilerParams(vmem_limit_bytes=VMEM_LIMIT),
        cost_estimate=pl.CostEstimate(flops=4 * nh * length * length * head_dim, transcendentals=0,
                                      bytes_accessed=8 * nh * length * head_dim),
        name='attention',
    )(bounds, qkv, qkv, qkv, segq, segk)


def out_kernel(columns, heads, parts, has_acc, *refs):
    n = len(parts)
    o_refs, w_ref, refs = refs[:n], refs[n], refs[n + 1:]
    acc_ref, refs = (refs[0], refs[1:]) if has_acc else (None, refs)
    y_ref, lhs, sem = refs
    batch, tokens = lhs.shape[:2]

    @pl.when(pl.program_id(0) == 0)
    def _():
        copies = []
        for seq in range(batch):
            at = 0
            for group in range(4):
                source = (seq // 2) * 8 + (group // 2) * 4 + (seq % 2) * 2 + group % 2
                for k in range(n):
                    size = o_refs[k].shape[2]
                    copies.append(pltpu.make_async_copy(o_refs[k].at[source], lhs.at[seq, :, pl.ds(at, size)], sem))
                    at += size
        for copy in copies:
            copy.start()
        for copy in copies:
            copy.wait()

    depth = lhs.shape[2]
    y = jnp.dot(lhs[...].reshape(batch * tokens, depth), w_ref[...].reshape(depth, w_ref.shape[-1]),
                preferred_element_type=jnp.float32)
    y = y.reshape(y_ref.shape)
    if has_acc:
        y = acc_ref[...] + y
    y_ref[...] = y.astype(y_ref.dtype)


def out_project(os, starts, w_out, acc, columns, heads, dtype, tile=512):
    n_heads, head_dim, width = w_out.shape
    tile = min(tile, width)
    n_blocks, tokens, _ = os[0].shape
    groups = n_heads // heads
    batch = n_blocks // groups
    count = sum(o.shape[2] for o in os) // head_dim
    first = starts[0]
    w = w_out.reshape(groups, heads, head_dim, width)
    w_spec = pl.BlockSpec(tuple(pl.Element(n) for n in (groups, count, head_dim, tile)), lambda i: (0, first, 0, i * tile))
    y_spec = pl.BlockSpec((batch, tokens, tile), lambda i: (0, 0, i))
    ins = [*os, w] + ([] if acc is None else [acc])
    return pl.pallas_call(
        functools.partial(out_kernel, columns, heads, starts, acc is not None),
        out_shape=jax.ShapeDtypeStruct((batch, tokens, width), dtype),
        grid=(width // tile,),
        in_specs=[pl.BlockSpec(memory_space=pl.ANY)] * len(os) + [w_spec] + ([] if acc is None else [y_spec]),
        out_specs=y_spec,
        scratch_shapes=[pltpu.VMEM((batch, tokens, groups * count * head_dim), jnp.bfloat16), pltpu.SemaphoreType.DMA],
        compiler_params=pltpu.CompilerParams(vmem_limit_bytes=VMEM_LIMIT),
        cost_estimate=pl.CostEstimate(flops=2 * batch * tokens * groups * count * head_dim * width, transcendentals=0,
                                      bytes_accessed=2 * groups * count * head_dim * width),
        name='out_project',
    )(*ins)


def solution(mesh):
    n_cp, n_sp = mesh.shape['cp'], mesh.shape['sp']
    n_blocks = n_cp * n_sp
    columns = n_cp // CORES
    token_spec = P('dp', ('cp', 'sp'), None)
    seg_spec = P('dp', ('cp', 'sp'))

    def local_layer(hidden, seg_ids, w_qkv, w_out):
        batch, tokens, depth = hidden.shape
        n_heads, head_dim = w_out.shape[:2]
        groups = n_blocks // batch
        assert n_sp == 4 and columns == 4 and groups == 4 and batch == 2 * columns
        heads = n_heads // groups
        x, core, pair, end = place(lax.axis_index('cp'), lax.axis_index('sp'))
        seq = x * 2 + pair
        qkv, seg = gather_project(hidden, seg_ids, w_qkv, heads, columns, n_blocks)
        seg = lax.dynamic_slice(seg, (0, seq, 0), (n_blocks, 1, tokens)).reshape(n_blocks * tokens)
        parts = ((0, heads // 3), (heads // 3, heads // 2), (heads - heads // 6, heads // 6))
        os = []
        for h0, nh in parts:
            o = attention(qkv, seg, heads, head_dim, 512, 512, h0, nh)
            o = o.reshape(n_blocks, tokens, nh * head_dim)
            os.append(lax.all_to_all(o, ('cp', 'sp'), 0, 0, tiled=True))
        starts = [h0 for h0, _ in parts]
        acc = out_project(os[:-1], starts[:-1], w_out, None, columns, heads, jnp.float32)
        return out_project(os[-1:], starts[-1:], w_out, acc, columns, heads, jnp.bfloat16)

    return jax.shard_map(local_layer, mesh=mesh, in_specs=(token_spec, seg_spec, P(), P()), out_specs=token_spec,
                         check_vma=False)
```

```python
import functools
import math

import jax
import jax.numpy as jnp
from jax import lax
from jax.experimental import pallas as pl
from jax.experimental.pallas import tpu as pltpu
from jax.sharding import PartitionSpec as P

MESH = pl.DeviceIdType.MESH
CORES = 2
VMEM_LIMIT = 67043328


def place(rank, lane):
    return rank // CORES, rank % CORES, lane // 2, lane % 2


def gather_project_kernel(columns, heads, hid, seg, w_hbm, out, seg_out, blocks, w_vmem, stage, w_in, w_wide, recv_sem,
                          direct_sem, relay_sem, twin_sem, w_sem, own_sem, out_sem, seg_send, seg_recv, transit, transit_recv,
                          transit_send):
    rank, lane = lax.axis_index('cp'), lax.axis_index('sp')
    x, core, pair, end = place(rank, lane)
    far = 3 - lane
    mate = 2 * pair + 1 - end
    n_blocks = blocks.shape[0]
    lanes = n_blocks // (columns * CORES)

    def dev(xx, cc, yy):
        return {'cp': xx * CORES + cc, 'sp': yy}

    def slot_of(xx, hh, cc, ee):
        return ((xx * 2 + hh) * CORES + cc) * 2 + ee

    me = slot_of(x, pair, core, end)
    n_groups = n_blocks // 4
    twin = dev(x, 1 - core, lane)
    partner = dev(x, core, mate)

    def peer(k):
        p = (rank * lanes + lane + k) % n_blocks
        return {'cp': p // lanes, 'sp': p % lanes}

    barrier = pltpu.get_barrier_semaphore()

    def greet(k, carry):
        pl.semaphore_signal(barrier, inc=1, device_id=peer(k), device_id_type=MESH)
        return carry

    lax.fori_loop(1, n_blocks, greet, 0)

    own = pltpu.make_async_copy(hid.at[x * 2 + pair], blocks.at[me], own_sem.at[0])
    own.start()
    here = rank * lanes + lane
    own_seg = pltpu.make_async_copy(seg, seg_out.at[here], own_sem.at[1])
    own_seg.start()

    first = (core * 2 + end) * heads
    tile0 = jnp.minimum(first // 8, w_hbm.shape[2] // 8 - 2) * 8
    shift = first - tile0
    depth, width = w_vmem.shape
    chunk = w_in.shape[1]

    def w_copy(n):
        return pltpu.make_async_copy(
            w_hbm.at[pl.ds(pl.multiple_of(n * chunk, chunk), chunk), :, pl.ds(pl.multiple_of(tile0, 8), 16), :],
            w_in.at[n % 2], w_sem.at[n % 2])

    w_copy(0).start()
    pl.semaphore_wait(barrier, n_blocks - 1)

    right, left = (x + 1) % columns, (x + columns - 1) % columns
    across = (x + 2) % columns
    directs = []
    sends = [(across * 2 + pair, transit.at[0], transit_recv.at[0], dev(right, core, lane)),
             (across * 2 + 1 - pair, transit.at[1], transit_recv.at[1], dev(left, core, lane))]
    for xt, other in ((x, 1), (left, 0), (right, 0), (left, 1), (right, 1)):
        sends.append((xt * 2 + (1 - pair if other else pair), blocks.at[me], recv_sem.at[me],
                      dev(xt, core, far if other else lane)))
    for i, (seq, place_, sem, device) in enumerate(sends):
        copy = pltpu.make_async_remote_copy(src_ref=hid.at[seq], dst_ref=place_, send_sem=direct_sem.at[i], recv_sem=sem,
                                            device_id=device, device_id_type=MESH)
        copy.start()
        directs.append(copy)

    passes = [
        pltpu.make_async_remote_copy(
            src_ref=transit.at[0], dst_ref=blocks.at[slot_of(left, pair, core, end)], send_sem=transit_send.at[0],
            recv_sem=recv_sem.at[slot_of(left, pair, core, end)], device_id=dev(right, core, lane), device_id_type=MESH),
        pltpu.make_async_remote_copy(
            src_ref=transit.at[1], dst_ref=blocks.at[slot_of(right, pair, core, end)], send_sem=transit_send.at[1],
            recv_sem=recv_sem.at[slot_of(right, pair, core, end)], device_id=dev(left, core, far), device_id_type=MESH)]
    arrivals = [pltpu.make_async_remote_copy(
        src_ref=transit.at[n], dst_ref=transit.at[n], send_sem=transit_send.at[n], recv_sem=transit_recv.at[n],
        device_id=twin, device_id_type=MESH) for n in range(2)]

    def remote(slot, sem, device):
        return pltpu.make_async_remote_copy(
            src_ref=blocks.at[slot], dst_ref=blocks.at[slot], send_sem=sem, recv_sem=recv_sem.at[slot],
            device_id=device, device_id_type=MESH)

    def group(j):
        s = j // 2
        dx = s + jnp.where(s == 2, 1, 0) - jnp.where(s == 3, 1, 0)
        return (x + dx) % columns, (pair + j % 2) % 2

    def sides(j):
        de = jnp.where(j % 2 == 0, end, 1 - end)
        return de, 1 - de

    def serve(j):
        xs, hs = group(j)
        slot = slot_of(xs, hs, core, sides(j)[0])

        @pl.when(j > 0)
        def _():
            remote(slot, relay_sem.at[j], partner).wait_recv()

        remote(slot, relay_sem.at[j], partner).start()
        remote(slot, twin_sem.at[j, 0], twin).start()

    own.wait()
    serve(0)

    def send_seg(k, carry):
        pltpu.make_async_remote_copy(src_ref=seg, dst_ref=seg_out.at[here], send_sem=seg_send, recv_sem=seg_recv,
                                     device_id=peer(k), device_id_type=MESH).start()
        return carry

    lax.fori_loop(1, n_blocks, send_seg, 0)

    n_chunks = depth // chunk
    lane_width = w_wide.shape[1]

    def relay_weights(n, carry):
        @pl.when(n + 1 < n_chunks)
        def _():
            w_copy(n + 1).start()

        w_copy(n).wait()
        half = chunk * 8
        for kind in range(3):
            both = w_in[n % 2, :, kind].astype(jnp.float32)
            for part in range(2):
                w_wide[pl.ds((2 * kind + part) * half, half), :] = both[:, part * 8:part * 8 + 8].reshape(half, lane_width)
        for kind in range(3):
            for h in range(heads):
                row = (2 * kind + (shift + h) // 8) * half + (shift + h) % 8
                at = (kind * heads + h) * lane_width
                w_vmem[pl.ds(pl.multiple_of(n * chunk, chunk), chunk), pl.ds(at, lane_width)] = (
                    w_wide[pl.ds(row, chunk, stride=8), :].astype(jnp.bfloat16))
        return carry

    lax.fori_loop(0, n_chunks // 2, relay_weights, 0)
    serve(1)
    lax.fori_loop(n_chunks // 2, n_chunks, relay_weights, 0)
    for arrival, copy in zip(arrivals, passes):
        arrival.wait_recv()
        copy.start()

    rows = stage.shape[1] // 4
    tile = 256

    def out_copies(j):
        xs, hs = group(j)
        buf = j % 2
        return [pltpu.make_async_copy(
            stage.at[buf, pl.ds(k * rows, rows)],
            out.at[pl.ds(pl.multiple_of(((xs * CORES + k // 2) * lanes + hs * 2 + k % 2) * rows, rows), rows)],
            out_sem.at[buf, k]) for k in range(4)]

    def step(j, carry):
        xs, hs = group(j)
        de, ve = sides(j)

        @pl.when(j + 2 < n_groups)
        def _():
            serve(j + 2)

        via = slot_of(xs, hs, core, ve)
        remote(via, twin_sem.at[j, 1], twin).wait_recv()
        remote(via, twin_sem.at[j, 1], twin).start()
        remote(slot_of(xs, hs, 1 - core, de), twin_sem.at[j, 0], twin).wait_recv()
        remote(slot_of(xs, hs, 1 - core, ve), twin_sem.at[j, 1], twin).wait_recv()

        @pl.when(j >= 2)
        def _():
            for copy in out_copies(j - 2):
                copy.wait()

        lhs = blocks.at[pl.ds(slot_of(xs, hs, 0, 0), 4)]
        buf = j % 2

        def column(n, carry):
            c = pl.ds(pl.multiple_of(n * tile, tile), tile)
            acc = jnp.dot(lhs[...].reshape(4 * rows, depth), w_vmem[:, c], preferred_element_type=jnp.float32)
            stage[buf, :, c] = acc.astype(jnp.bfloat16)
            return carry

        lax.fori_loop(0, width // tile, column, 0)
        for copy in out_copies(j):
            copy.start()
        return carry

    lax.fori_loop(0, n_groups, step, 0)

    for copy in directs + passes:
        copy.wait_send()

    def drain(j, carry):
        remote(me, relay_sem.at[j], partner).wait_send()
        remote(me, twin_sem.at[j, 0], twin).wait_send()
        remote(me, twin_sem.at[j, 1], twin).wait_send()

        @pl.when(j >= n_groups - 2)
        def _():
            for copy in out_copies(j):
                copy.wait()

        return carry

    lax.fori_loop(0, n_groups, drain, 0)
    others = seg_out.at[pl.ds(0, n_blocks - 1)]
    all_segs = pltpu.make_async_remote_copy(src_ref=others, dst_ref=others, send_sem=seg_send, recv_sem=seg_recv,
                                            device_id=twin, device_id_type=MESH)
    all_segs.wait_send()
    all_segs.wait_recv()
    own_seg.wait()


def gather_project(hidden, seg_ids, w_qkv, heads, columns, n_blocks):
    batch, tokens, depth = hidden.shape
    head_dim = w_qkv.shape[3]
    width = 3 * heads * head_dim
    n_groups = n_blocks // 4
    chunk = 64 if depth % 128 == 0 else depth
    return pl.pallas_call(
        functools.partial(gather_project_kernel, columns, heads),
        out_shape=(jax.ShapeDtypeStruct((n_blocks * tokens, width), jnp.bfloat16),
                   jax.ShapeDtypeStruct((n_blocks,) + seg_ids.shape, seg_ids.dtype)),
        in_specs=[pl.BlockSpec(memory_space=pl.ANY)] * 3,
        out_specs=[pl.BlockSpec(memory_space=pl.ANY)] * 2,
        scratch_shapes=[
            pltpu.VMEM((n_blocks, tokens, depth), jnp.bfloat16),
            pltpu.VMEM((depth, width), jnp.bfloat16),
            pltpu.VMEM((2, 4 * tokens, width), jnp.bfloat16),
            pltpu.VMEM((2, chunk, 3, 16, head_dim), jnp.bfloat16),
            pltpu.VMEM((3 * 16 * chunk, head_dim), jnp.float32),
            pltpu.SemaphoreType.DMA((n_blocks,)),
            pltpu.SemaphoreType.DMA((n_groups - 1,)),
            pltpu.SemaphoreType.DMA((n_groups,)),
            pltpu.SemaphoreType.DMA((n_groups, 2)),
            pltpu.SemaphoreType.DMA((2,)),
            pltpu.SemaphoreType.DMA((2,)),
            pltpu.SemaphoreType.DMA((2, 4)),
            pltpu.SemaphoreType.DMA,
            pltpu.SemaphoreType.DMA,
            pltpu.VMEM((2, tokens, depth), jnp.bfloat16),
            pltpu.SemaphoreType.DMA((2,)),
            pltpu.SemaphoreType.DMA((2,)),
        ],
        compiler_params=pltpu.CompilerParams(collective_id=0, has_side_effects=True, vmem_limit_bytes=VMEM_LIMIT),
        name='gather_project',
    )(hidden, seg_ids, w_qkv)


def attention_kernel(tk, scale2, bounds, q_ref, k_ref, v_ref, segq_ref, segk_ref, o_ref, vt, s_even, s_odd, acc):
    i = pl.program_id(1)
    tq, head_dim = q_ref.shape

    @pl.when(i == 0)
    def _():
        vt[...] = v_ref[...].T

    lo, full_lo, full_hi, hi = (bounds[n, i] for n in range(4))
    q = q_ref[...]
    last_chunk = k_ref.shape[0] // tk - 1
    head = full_lo - lo
    n_edge, n_full = head + hi - full_hi, full_hi - full_lo

    def at(chunk):
        return pl.ds(pl.multiple_of(chunk * tk, tk), tk)

    def edge(n):
        return jnp.minimum(jnp.where(n < head, lo + n, full_hi + n - head), last_chunk)

    def scores(chunk, s_ref, masked):
        s = lax.dot_general(k_ref[at(chunk), :], q, (((1,), (1,)), ((), ())), preferred_element_type=jnp.float32)
        if masked:
            segk = segk_ref[at(chunk), :]
            allowed = jnp.concatenate([segk] * (tq // segk.shape[1]), axis=1) == segq_ref[:1, :]
            s = jnp.where(allowed, s, -jnp.inf)
        s_ref[...] = s
        return jnp.max(s, axis=0, keepdims=True)

    def absorb(chunk, s, top, m, l):
        m_new = jnp.maximum(m, top)
        p = jnp.exp2((s - m_new) * scale2)
        alpha = jnp.exp2((m - m_new) * scale2)
        l = l * alpha + jnp.sum(p, axis=0, keepdims=True)
        acc[...] = acc[...] * alpha + lax.dot_general(vt[:, at(chunk)], p.astype(jnp.bfloat16), (((1,), (0,)), ((), ())),
                                                      preferred_element_type=jnp.float32)
        return m_new, l

    def run(count, chunk_of, masked, m, l):
        def pair_step(n, state):
            m, l, top_even = state
            n = 2 * n
            top_odd = scores(chunk_of(n + 1), s_odd, masked)
            m, l = absorb(chunk_of(n), s_even[...], top_even, m, l)
            top_even = scores(chunk_of(n + 2), s_even, masked)
            m, l = absorb(chunk_of(n + 1), s_odd[...], top_odd, m, l)
            return m, l, top_even

        def odd(n, state):
            top = scores(chunk_of(0), s_even, masked)
            m, l, top = lax.fori_loop(0, count // 2, pair_step, (*state, top))
            return lax.fori_loop(0, count % 2, lambda n, state: absorb(chunk_of(count - 1), s_even[...], top, *state), (m, l))

        return lax.fori_loop(0, jnp.minimum(count, 1), odd, (m, l))

    acc[...] = jnp.zeros_like(acc)
    m, l = jnp.full((1, tq), jnp.finfo(jnp.float32).min, jnp.float32), jnp.zeros((1, tq), jnp.float32)
    m, l = run(n_edge, edge, True, m, l)
    m, l = run(n_full, lambda n: jnp.minimum(full_lo + n, last_chunk), False, m, l)
    o_ref[...] = (acc[...] / l).T.astype(o_ref.dtype)


def attention(qkv, seg, heads, head_dim, tq, tk, h0, nh):
    length = qkv.shape[0]
    n_q = length // tq
    first, last = seg[::tq], seg[tq - 1::tq]
    start = jnp.sum(seg[None, :] < first[:, None], axis=1)
    stop = jnp.sum(seg[None, :] <= last[:, None], axis=1)
    lo, hi = start // tk, (stop + tk - 1) // tk
    full_lo, full_hi = (start + tk - 1) // tk, stop // tk
    plain = (first == last) & (full_hi > full_lo)
    bounds = jnp.stack([lo, jnp.where(plain, full_lo, hi), jnp.where(plain, full_hi, hi), hi]).astype(jnp.int32)
    segq = jnp.broadcast_to(seg[None, :], (8, length))
    segk = jnp.broadcast_to(seg[:, None], (length, 128))
    scale2 = head_dim ** -0.5 * math.log2(math.e)
    return pl.pallas_call(
        functools.partial(attention_kernel, tk, scale2),
        out_shape=jax.ShapeDtypeStruct((length, nh * head_dim), jnp.bfloat16),
        grid_spec=pltpu.PrefetchScalarGridSpec(
            num_scalar_prefetch=1, grid=(nh, n_q),
            in_specs=[
                pl.BlockSpec((tq, head_dim), lambda h, i, b: (i, h0 + h)),
                pl.BlockSpec((length, head_dim), lambda h, i, b: (0, heads + h0 + h)),
                pl.BlockSpec((length, head_dim), lambda h, i, b: (0, 2 * heads + h0 + h)),
                pl.BlockSpec((8, tq), lambda h, i, b: (0, i)),
                pl.BlockSpec((length, 128), lambda h, i, b: (0, 0)),
            ],
            out_specs=pl.BlockSpec((tq, head_dim), lambda h, i, b: (i, h)),
            scratch_shapes=[
                pltpu.VMEM((head_dim, length), jnp.bfloat16),
                pltpu.VMEM((tk, tq), jnp.float32),
                pltpu.VMEM((tk, tq), jnp.float32),
                pltpu.VMEM((head_dim, tq), jnp.float32),
            ]),
        compiler_params=pltpu.CompilerParams(vmem_limit_bytes=VMEM_LIMIT),
        cost_estimate=pl.CostEstimate(flops=4 * nh * length * length * head_dim, transcendentals=0,
                                      bytes_accessed=8 * nh * length * head_dim),
        name='attention',
    )(bounds, qkv, qkv, qkv, segq, segk)


def out_kernel(columns, heads, parts, has_acc, *refs):
    n = len(parts)
    o_refs, w_ref, refs = refs[:n], refs[n], refs[n + 1:]
    acc_ref, refs = (refs[0], refs[1:]) if has_acc else (None, refs)
    y_ref, lhs, sem = refs
    batch, tokens = lhs.shape[:2]

    @pl.when(pl.program_id(0) == 0)
    def _():
        copies = []
        for seq in range(batch):
            at = 0
            for group in range(4):
                source = (seq // 2) * 8 + (group // 2) * 4 + (seq % 2) * 2 + group % 2
                for k in range(n):
                    size = o_refs[k].shape[2]
                    copies.append(pltpu.make_async_copy(o_refs[k].at[source], lhs.at[seq, :, pl.ds(at, size)], sem))
                    at += size
        for copy in copies:
            copy.start()
        for copy in copies:
            copy.wait()

    depth = lhs.shape[2]
    y = jnp.dot(lhs[...].reshape(batch * tokens, depth), w_ref[...].reshape(depth, w_ref.shape[-1]),
                preferred_element_type=jnp.float32)
    y = y.reshape(y_ref.shape)
    if has_acc:
        y = acc_ref[...] + y
    y_ref[...] = y.astype(y_ref.dtype)


def out_project(os, starts, w_out, acc, columns, heads, dtype, tile=512):
    n_heads, head_dim, width = w_out.shape
    tile = min(tile, width)
    n_blocks, tokens, _ = os[0].shape
    groups = n_heads // heads
    batch = n_blocks // groups
    count = sum(o.shape[2] for o in os) // head_dim
    first = starts[0]
    w = w_out.reshape(groups, heads, head_dim, width)
    w_spec = pl.BlockSpec(tuple(pl.Element(n) for n in (groups, count, head_dim, tile)), lambda i: (0, first, 0, i * tile))
    y_spec = pl.BlockSpec((batch, tokens, tile), lambda i: (0, 0, i))
    ins = [*os, w] + ([] if acc is None else [acc])
    return pl.pallas_call(
        functools.partial(out_kernel, columns, heads, starts, acc is not None),
        out_shape=jax.ShapeDtypeStruct((batch, tokens, width), dtype),
        grid=(width // tile,),
        in_specs=[pl.BlockSpec(memory_space=pl.ANY)] * len(os) + [w_spec] + ([] if acc is None else [y_spec]),
        out_specs=y_spec,
        scratch_shapes=[pltpu.VMEM((batch, tokens, groups * count * head_dim), jnp.bfloat16), pltpu.SemaphoreType.DMA],
        compiler_params=pltpu.CompilerParams(vmem_limit_bytes=VMEM_LIMIT),
        cost_estimate=pl.CostEstimate(flops=2 * batch * tokens * groups * count * head_dim * width, transcendentals=0,
                                      bytes_accessed=2 * groups * count * head_dim * width),
        name='out_project',
    )(*ins)


def solution(mesh):
    n_cp, n_sp = mesh.shape['cp'], mesh.shape['sp']
    n_blocks = n_cp * n_sp
    columns = n_cp // CORES
    token_spec = P('dp', ('cp', 'sp'), None)
    seg_spec = P('dp', ('cp', 'sp'))

    def local_layer(hidden, seg_ids, w_qkv, w_out):
        batch, tokens, depth = hidden.shape
        n_heads, head_dim = w_out.shape[:2]
        groups = n_blocks // batch
        assert n_sp == 4 and columns == 4 and groups == 4 and batch == 2 * columns
        heads = n_heads // groups
        x, core, pair, end = place(lax.axis_index('cp'), lax.axis_index('sp'))
        seq = x * 2 + pair
        qkv, seg = gather_project(hidden, seg_ids, w_qkv, heads, columns, n_blocks)
        seg = lax.dynamic_slice(seg, (0, seq, 0), (n_blocks, 1, tokens)).reshape(n_blocks * tokens)
        parts = tuple((n * heads // 3, heads // 3) for n in range(3))
        os = []
        for h0, nh in parts:
            o = attention(qkv, seg, heads, head_dim, 512, 512, h0, nh)
            o = o.reshape(n_blocks, tokens, nh * head_dim)
            os.append(lax.all_to_all(o, ('cp', 'sp'), 0, 0, tiled=True))
        starts = [h0 for h0, _ in parts]
        acc = out_project(os[:-1], starts[:-1], w_out, None, columns, heads, jnp.float32)
        return out_project(os[-1:], starts[-1:], w_out, acc, columns, heads, jnp.bfloat16)

    return jax.shard_map(local_layer, mesh=mesh, in_specs=(token_spec, seg_spec, P(), P()), out_specs=token_spec,
                         check_vma=False)
```
